32 devices in a mesh: dp: 1, sp: 32 (over x, y, z, core).
Axes of the slice: x: 2, y: 2, z: 4, core: 2. Of those that a mesh axis runs over, the one named last changes fastest.
Arguments:
- x: bfloat16 [8192, 2048], P(('dp', 'sp'))
- gain: bfloat16 [2048], replicated
- wq: bfloat16 [2048, 2048], replicated
- wk: bfloat16 [2048, 256], replicated
- wv: bfloat16 [2048, 256], replicated
- wo: bfloat16 [2048, 2048], replicated
Outputs:
- output: bfloat16 [8192, 2048], P(('dp', 'sp'))
All inputs are finite; a program needn't handle non-finite values.
Results may differ from the reference program's by a relative error of at most 0.012.
Values are sent between devices in bfloat16 or wider.
A program may use at most 2 GiB of HBM per device.

```python
import jax
import jax.numpy as jnp
from jax import lax

ROWS = 8192
D = 2048
HEADS = 8
KV_HEADS = 1
HEAD = 256
THETA = 10000


def setup_inputs(seed: int = 0, part: int = 0) -> dict:
    kx, kn, kq, kk, kv, ko = jax.random.split(jax.random.key(seed), 6)

    def weights(key, rows, columns):
        return jax.random.normal(key, (rows, columns), jnp.float32) * rows**-0.5

    drawn = {
        "x": jax.random.normal(jax.random.fold_in(kx, part), (ROWS, D), jnp.float32),
        "gain": 1 + 0.1 * jax.random.normal(kn, (D,), jnp.float32),
        "wq": 2 * weights(kq, D, HEADS * HEAD),
        "wk": 2 * weights(kk, D, KV_HEADS * HEAD),
        "wv": 4 * weights(kv, D, KV_HEADS * HEAD),
        "wo": weights(ko, HEADS * HEAD, D),
    }
    return {k: v.astype(jnp.bfloat16) for k, v in drawn.items()}


def normed(x, gain):
    wide = x.astype(jnp.float32)
    scale = lax.rsqrt(jnp.mean(wide * wide, -1, keepdims=True) + 1e-6)
    return (wide * scale * gain.astype(jnp.float32)).astype(jnp.bfloat16)


def turned(t, place, theta):
    half = t.shape[-1] // 2
    angle = place.astype(jnp.float32)[:, None] * theta ** (-jnp.arange(half, dtype=jnp.float32) / half)
    cos, sin = jnp.cos(angle)[:, None], jnp.sin(angle)[:, None]
    a, b = t[..., :half].astype(jnp.float32), t[..., half:].astype(jnp.float32)
    return jnp.concatenate([a * cos - b * sin, b * cos + a * sin], -1).astype(jnp.bfloat16)


def matmul(a, w):
    return jnp.dot(a, w, preferred_element_type=jnp.float32).astype(jnp.bfloat16)


def einsum(form, a, b):
    return jnp.einsum(form, a.astype(jnp.float32), b.astype(jnp.float32))


def attention(q, k, v):
    scores = einsum("tgsd,ugd->gstu", q, k) * q.shape[-1] ** -0.5
    token = jnp.arange(q.shape[0])
    scores = jnp.where(token[:, None] >= token, scores, -jnp.inf)
    weights = jax.nn.softmax(scores, -1).astype(jnp.bfloat16)
    return einsum("gstu,ugd->tgsd", weights, v).astype(jnp.bfloat16)


def reference(x, gain, wq, wk, wv, wo):
    a, place = normed(x, gain), jnp.arange(ROWS)
    q = turned(matmul(a, wq).reshape(ROWS, HEADS, HEAD), place, THETA).reshape(ROWS, KV_HEADS, -1, HEAD)
    k = turned(matmul(a, wk).reshape(ROWS, KV_HEADS, HEAD), place, THETA)
    v = matmul(a, wv).reshape(ROWS, KV_HEADS, HEAD)
    seen = attention(q, k, v).reshape(ROWS, HEADS * HEAD)
    return (x.astype(jnp.float32) + jnp.dot(seen, wo, preferred_element_type=jnp.float32)).astype(jnp.bfloat16)
```

```python
import functools

import jax
import jax.numpy as jnp
import numpy as np
from jax import lax
from jax.experimental import pallas as pl
from jax.experimental.pallas import tpu as pltpu
from jax.sharding import PartitionSpec as P

D = 2048
HEADS = 8
HEAD = 256
HALF = 128
OWN = 256
DEVICES = 32
THETA = 10000
NEG = -1e30
HIDDEN = 2 * NEG
E = HEAD**-0.5 * 1.4426950408889634
COLS = HEADS * OWN
STRIP = 512

ORDER = {
    "X": (0, 2, 3, 1, 19, 6, 17, 7, 5, 21, 10, 23, 11, 9, 25, 14, 27, 15, 13, 29, 31),
    "Y": (0, 3, 1, 2, 32, 34, 6, 4, 7, 36, 8, 38, 10, 11, 40, 42, 14, 15, 12, 46, 44),
    "Z": (0, 2, 1, 3, 32, 4, 17, 6, 7, 36, 5, 21, 10, 11, 8, 9, 25, 40),
}

LATENCY = {"X": 3.0, "Y": 3.0, "Z": 3.9}


def _arrives_as(link, rel):
    return rel[0] ^ (link == "X"), rel[1] ^ (link == "Y"), (rel[2] + (link == "Z")) % 4


def _planned():
    left = {link: [((n // 32, n // 16 % 2, n // 4 % 4), n % 4) for n in order] for link, order in ORDER.items()}
    free = dict.fromkeys(ORDER, 0.0)
    here = {((0, 0, 0), p): 0.0 for p in range(4)}
    copies = []
    while any(left.values()):
        for link, rest in left.items():
            if rest and rest[0] in here:
                rel, p = rest.pop(0)
                start = max(free[link], here[rel, p])
                free[link] = start + 1
                here[_arrives_as(link, rel), p] = start + 1 + LATENCY[link]
                copies.append((link, rel, p, start, start + 1 + LATENCY[link]))
    return sorted(copies, key=lambda c: c[3])


COPIES = _planned()


def _events():
    events, came = [], {}
    for i, (link, rel, p, start, arrive) in enumerate(COPIES):
        came[_arrives_as(link, rel), p] = (arrive, i)
    for i, (link, rel, p, start, arrive) in enumerate(COPIES):
        ready = came[rel, p][0] if (rel, p) in came else 0.0
        events.append((max(ready, start - AHEAD), 1, start, i))
    for arrive, i in came.values():
        events.append((arrive, 0, arrive, i))
    return sorted(events), came


AHEAD = 4.0
EVENTS, CAME = _events()
RELS = sorted({rel for rel, _ in CAME}, key=lambda rel: (max(CAME[rel, p][0] for p in range(4)), rel))
T_QUERIES, T_FIRST, T_STEP = 0.5, 2.8, 1.2


def _slots():
    times = [T_QUERIES * i for i in range(4)] + [T_FIRST + T_STEP * i for i in range(len(RELS))]
    slots, at, got = [], 0, set()
    for n, t in enumerate(times):
        slot = []
        need = {CAME[RELS[n - 4], p][1] for p in range(4)} if n >= 4 else set()
        while at < len(EVENTS) and (EVENTS[at][0] <= t or not need <= got):
            slot.append(EVENTS[at])
            if EVENTS[at][1] == 0:
                got.add(EVENTS[at][3])
            at += 1
        slots.append(slot)
    return slots + [EVENTS[at:]]


def _dot(a, b, ca, cb):
    return lax.dot_general(a, b, (((ca,), (cb,)), ((), ())), preferred_element_type=jnp.float32)


def _turn(t, cos, sin):
    t = t.astype(jnp.bfloat16).astype(jnp.float32)
    a, b = t[:, :HALF], t[:, HALF:]
    return jnp.concatenate([a * cos - b * sin, b * cos + a * sin], axis=1).astype(jnp.bfloat16)


class _Ring:
    def __init__(self, kv, s_link, r_link, s_pair, r_pair):
        self.kv, self.s_link, self.r_link, self.s_pair, self.r_pair = kv, s_link, r_link, s_pair, r_pair
        me = lax.axis_index("sp")
        self.me, self.chip, self.core = me, me // 2, me % 2
        self.z, self.y, self.x = (me // 2) % 4, (me // 8) % 2, me // 16
        self.to = {"X": (me + 16) % 32, "Y": (me // 16) * 16 + (me + 8) % 16, "Z": (me // 8) * 8 + (me + 2) % 8}
        self.before = (me // 8) * 8 + (me + 6) % 8
        self.pair = me + 1 - 2 * self.core

    def chip_of(self, rel):
        return ((self.x + rel[0]) % 2) * 8 + ((self.y + rel[1]) % 2) * 4 + (self.z + 4 - rel[2]) % 4

    def piece(self, chip, core, p):
        return self.kv.at[chip * 2 + core, pl.ds(p * 128, 128), :]

    def greet(self):
        barrier = pltpu.get_barrier_semaphore()
        for d in (self.to["X"], self.to["Y"], self.to["Z"], self.before, self.pair):
            pl.semaphore_signal(barrier, inc=1, device_id={"sp": d})

    def greeted(self):
        pl.semaphore_wait(pltpu.get_barrier_semaphore(), 5)

    def link(self, i):
        link, rel, p, _, _ = COPIES[i]
        ref = self.piece(self.chip_of(rel), self.core, p)
        return pltpu.make_async_remote_copy(ref, ref, self.s_link.at[i], self.r_link.at[i], device_id={"sp": self.to[link]})

    def came(self, i):
        link, rel, p, _, _ = COPIES[i]
        ref = self.piece(self.chip_of(_arrives_as(link, rel)), self.core, p)
        return pltpu.make_async_remote_copy(ref, ref, self.s_link.at[i], self.r_link.at[i], device_id={"sp": self.to[link]})

    def across(self, rel, p, core):
        i = (rel[0] * 8 + rel[1] * 4 + rel[2]) * 4 + p
        ref = self.piece(self.chip_of(rel), core, p)
        return pltpu.make_async_remote_copy(ref, ref, self.s_pair.at[i], self.r_pair.at[i], device_id={"sp": self.pair})

    def run(self, slot):
        for _, kind, _, i in slot:
            if kind == 1:
                self.link(i).start()
            else:
                self.came(i).wait_recv()
                link, rel, p, _, _ = COPIES[i]
                self.across(_arrives_as(link, rel), p, self.core).start()


def _attend(kv, vt_s, q_s, top_s, mix_s, chip, visible):
    k = jnp.concatenate([kv[2 * chip, 0:256, :], kv[2 * chip + 1, 0:256, :]], axis=0)
    ones = jnp.ones((8, 512), jnp.bfloat16)
    vt = jnp.concatenate([jnp.concatenate([kv[2 * chip, 256:512, :].T, kv[2 * chip + 1, 256:512, :].T], axis=1), ones], axis=0)
    pieces = range(0, COLS, STRIP)
    scores = [_dot(k, q_s[at : at + STRIP, :], 1, 1) for at in pieces]
    weights, keeps = [], []
    for at, s in zip(pieces, scores):
        if visible is not None:
            s = jnp.where(visible, s, HIDDEN)
        old = top_s[0:1, at : at + STRIP]
        top = jnp.maximum(old, s.max(axis=0, keepdims=True))
        top_s[0:1, at : at + STRIP] = top
        weights.append(jnp.exp2((s - top) * E).astype(jnp.bfloat16))
        keeps.append(jnp.exp2((old - top) * E))
    for at, p, keep in zip(pieces, weights, keeps):
        mix_s[:, at : at + STRIP] = mix_s[:, at : at + STRIP] * keep + _dot(vt, p, 1, 0)


def _kernel(x_h, gain_h, wq_h, wk_h, wv_h, wo_h, cos_h, sin_h, base_h, y_ref,
            x_s, gain_s, wq_s, wkv_s, wo_s, cos_s, sin_s, base_s, a_s, q_s, seen_s, kv, top_s, mix_s, in_sem, s_link, r_link, s_pair, r_pair):
    ring = _Ring(kv, s_link, r_link, s_pair, r_pair)
    me = ring.me
    ring.greet()
    first = [(x_h, x_s), (gain_h, gain_s), (wk_h, wkv_s.at[:, pl.ds(0, HEAD)]), (wv_h, wkv_s.at[:, pl.ds(HEAD, HEAD)]),
             (cos_h, cos_s), (sin_h, sin_s), (base_h, base_s)]
    later = [(wq_h.at[:, pl.ds(512 * i, 512)], wq_s.at[:, pl.ds(512 * i, 512)]) for i in range(4)] + [(wo_h, wo_s)]
    first, later = ([pltpu.make_async_copy(a, b, in_sem.at[n + i]) for i, (a, b) in enumerate(c)] for n, c in ((0, first), (7, later)))
    for c in first:
        c.start()
    for c in first:
        c.wait()
    for c in later[:4]:
        c.start()

    wide = x_s[...].astype(jnp.float32)
    scale = lax.rsqrt(jnp.mean(wide * wide, -1, keepdims=True) + 1e-6)
    a_s[...] = (wide * scale * gain_s[...].astype(jnp.float32)[None]).astype(jnp.bfloat16)
    here = base_s[me]
    cb, sb = here[:, :HALF], here[:, HALF:]
    cos = cb * cos_s[...] - sb * sin_s[...]
    sin = sb * cos_s[...] + cb * sin_s[...]
    cos_s[...] = cos
    sin_s[...] = sin
    both = _dot(a_s[...], wkv_s[...], 1, 0)
    kv[me, 0:256, :] = _turn(both[:, :HEAD], cos, sin)
    kv[me, 256:512, :] = both[:, HEAD:].astype(jnp.bfloat16)

    ring.greeted()
    for p in range(4):
        ring.across((0, 0, 0), p, ring.core).start()
    slots = _slots()
    for i in range(4):
        ring.run(slots[i])
        later[i].wait()
        if i == 0:
            later[4].start()
        for h in (2 * i, 2 * i + 1):
            q = _dot(a_s[...], wq_s[:, h * HEAD : (h + 1) * HEAD], 1, 0)
            q_s[h * OWN : (h + 1) * OWN, :] = _turn(q, cos_s[...], sin_s[...])

    ring.run(slots[4])
    top_s[...] = jnp.full(top_s.shape, NEG, jnp.float32)
    mix_s[...] = jnp.zeros(mix_s.shape, jnp.float32)
    for p in range(4):
        ring.across((0, 0, 0), p, 1 - ring.core).wait_recv()
    place = ring.core * OWN + lax.rem(lax.broadcasted_iota(jnp.int32, (512, STRIP), 1), OWN)
    _attend(kv, None, q_s, top_s, mix_s, ring.chip, place >= lax.broadcasted_iota(jnp.int32, (512, STRIP), 0))

    def step(n, _):
        chip = 0
        for i, rel in enumerate(RELS):
            @pl.when(n == i)
            def _():
                ring.run(slots[5 + i])
                for p in range(4):
                    ring.across(rel, p, 1 - ring.core).wait_recv()
            chip = jnp.where(n == i, ring.chip_of(rel), chip)

        @pl.when(chip < ring.chip)
        def _():
            _attend(kv, None, q_s, top_s, mix_s, chip, None)

    lax.fori_loop(0, len(RELS), step, None)

    for h in range(HEADS):
        at = slice(h * OWN, (h + 1) * OWN)
        part = mix_s[:HEAD, at] * (1 / mix_s[HEAD : HEAD + 1, at])
        seen_s[:, h * HEAD : (h + 1) * HEAD] = part.astype(jnp.bfloat16).T
    later[4].wait()
    for at in range(0, D, 512):
        y = _dot(seen_s[...], wo_s[:, at : at + 512], 1, 0)
        y_ref[:, at : at + 512] = (x_s[:, at : at + 512].astype(jnp.float32) + y).astype(jnp.bfloat16)
    for i in range(len(COPIES)):
        ring.link(i).wait_send()
    for rel in [(0, 0, 0), *RELS]:
        for p in range(4):
            ring.across(rel, p, ring.core).wait_send()


def _tables():
    freq = THETA ** (-np.arange(HALF) / HALF)
    place = np.arange(OWN)[:, None] * freq
    start = (np.arange(DEVICES) * OWN)[:, None] * freq
    base = np.concatenate([np.cos(start), np.sin(start)], axis=1)[:, None]
    return [jnp.asarray(t, jnp.float32) for t in (np.cos(place), np.sin(place), base)]


def solution(mesh):
    def step(x, gain, wq, wk, wv, wo):
        vmem = lambda *shape: pltpu.VMEM(shape, jnp.bfloat16)
        wide = lambda *shape: pltpu.VMEM(shape, jnp.float32)
        dma = pltpu.SemaphoreType.DMA
        return pl.pallas_call(
            _kernel,
            out_shape=jax.ShapeDtypeStruct((OWN, D), jnp.bfloat16),
            in_specs=[pl.BlockSpec(memory_space=pl.ANY)] * 9,
            out_specs=pl.BlockSpec(memory_space=pltpu.VMEM),
            scratch_shapes=[vmem(OWN, D), vmem(D), vmem(D, D), vmem(D, 2 * HEAD), vmem(D, D), wide(OWN, HALF), wide(OWN, HALF),
                            wide(DEVICES, 1, HEAD), vmem(OWN, D), vmem(COLS, HEAD), vmem(OWN, D), vmem(DEVICES, 2 * OWN, HEAD),
                            wide(8, COLS), wide(HEAD + 8, COLS), dma((12,)), dma((len(COPIES),)), dma((len(COPIES),)), dma((64,)), dma((64,))],
            compiler_params=pltpu.CompilerParams(collective_id=0, has_side_effects=True, vmem_limit_bytes=60 * 2**20),
            name="layer",
        )(x, gain, wq, wk, wv, wo, *_tables())

    tokens, whole = P(("dp", "sp"), None), P(None, None)
    return jax.shard_map(step, mesh=mesh, in_specs=(tokens, P(None), whole, whole, whole, whole), out_specs=tokens, check_vma=False)
```

```python
import functools

import jax
import jax.numpy as jnp
import numpy as np
from jax import lax
from jax.experimental import pallas as pl
from jax.experimental.pallas import tpu as pltpu
from jax.sharding import PartitionSpec as P

D = 2048
HEADS = 8
HEAD = 256
HALF = 128
OWN = 256
DEVICES = 32
THETA = 10000
NEG = -1e30
HIDDEN = 2 * NEG
E = HEAD**-0.5 * 1.4426950408889634
COLS = HEADS * OWN

ORDER = {
    "X": (2, 0, 3, 1, 17, 19, 6, 7, 5, 21, 10, 23, 11, 9, 25, 14, 27, 15, 13, 29, 31),
    "Y": (1, 3, 2, 0, 34, 6, 7, 4, 32, 10, 38, 36, 11, 8, 42, 14, 40, 15, 46, 12, 44),
    "Z": (2, 3, 0, 1, 17, 6, 7, 32, 4, 5, 21, 10, 36, 11, 9, 8, 25, 40),
}

LATENCY = {"X": 2.81, "Y": 2.81, "Z": 3.71}


def _arrives_as(link, rel):
    return rel[0] ^ (link == "X"), rel[1] ^ (link == "Y"), (rel[2] + (link == "Z")) % 4


def _planned():
    left = {link: [((n // 32, n // 16 % 2, n // 4 % 4), n % 4) for n in order] for link, order in ORDER.items()}
    free = dict.fromkeys(ORDER, 0.0)
    here = {((0, 0, 0), p): 0.0 for p in range(4)}
    copies = []
    while any(left.values()):
        for link, rest in left.items():
            if rest and rest[0] in here:
                rel, p = rest.pop(0)
                start = max(free[link], here[rel, p])
                free[link] = start + 1
                here[_arrives_as(link, rel), p] = start + 1 + LATENCY[link]
                copies.append((link, rel, p, start, start + 1 + LATENCY[link]))
    return sorted(copies, key=lambda c: c[3])


COPIES = _planned()


def _events():
    events, came = [], {}
    for i, (link, rel, p, start, arrive) in enumerate(COPIES):
        came[_arrives_as(link, rel), p] = (arrive, i)
    for i, (link, rel, p, start, arrive) in enumerate(COPIES):
        ready = came[rel, p][0] if (rel, p) in came else 0.0
        events.append((max(ready, start - AHEAD), 1, start, i))
    for (rel, p), (arrive, i) in came.items():
        onward = any(c[1:3] == (rel, p) for c in COPIES)
        events.append((arrive if onward else arrive + LATE, 0, arrive, i))
    return sorted(events), came


def _from(chip, rel):
    return (chip // 8 + rel[0]) % 2 * 8 + (chip // 4 + rel[1]) % 2 * 4 + (chip + 4 - rel[2]) % 4


def _next(chip, link):
    step = {"X": (1, 0, 0), "Y": (0, 1, 0), "Z": (0, 0, 3)}[link]
    return _from(chip, step)


def _used():
    @functools.cache
    def used(chip, i):
        link, rel, p, _, _ = COPIES[i]
        to, came = _next(chip, link), _arrives_as(link, rel)
        on = [j for j, c in enumerate(COPIES) if c[1:3] == (came, p)]
        return _from(chip, rel) < to or any(used(to, j) for j in on)

    sends, gets = [0] * len(COPIES), [0] * len(COPIES)
    for i, copy in enumerate(COPIES):
        for chip in range(16):
            if used(chip, i):
                sends[i] |= 1 << chip
                gets[i] |= 1 << _next(chip, copy[0])
    return sends, gets


SENDS, GETS = _used()
AHEAD = 1
LATE = 0.5
EVENTS, CAME = _events()
RELS = sorted({rel for rel, _ in CAME}, key=lambda rel: (max(CAME[rel, p][0] for p in range(4)), rel))
T_QUERIES, T_FIRST, T_STEP = 0.5, 4.34, 1.17


def _slots():
    times = [T_QUERIES * i for i in range(4)] + [T_FIRST + T_STEP * i for i in range(len(RELS))]
    slots, at, got = [], 0, set()
    for n, t in enumerate(times):
        slot = []
        need = {CAME[RELS[n - 4], p][1] for p in range(4)} if n >= 4 else set()
        while at < len(EVENTS) and (EVENTS[at][0] <= t or not need <= got):
            slot.append(EVENTS[at])
            if EVENTS[at][1] == 0:
                got.add(EVENTS[at][3])
            at += 1
        slots.append(slot)
    return slots + [EVENTS[at:]]


def _dot(a, b, ca, cb):
    return lax.dot_general(a, b, (((ca,), (cb,)), ((), ())), preferred_element_type=jnp.float32)


def _turn(t, cos, sin):
    t = t.astype(jnp.bfloat16).astype(jnp.float32)
    a, b = t[:, :HALF], t[:, HALF:]
    return jnp.concatenate([a * cos - b * sin, b * cos + a * sin], axis=1).astype(jnp.bfloat16)


class _Ring:
    def __init__(self, kv, s_link, r_link, s_pair, r_pair):
        self.kv, self.s_link, self.r_link, self.s_pair, self.r_pair = kv, s_link, r_link, s_pair, r_pair
        me = lax.axis_index("sp")
        self.me, self.chip, self.core = me, me // 2, me % 2
        self.z, self.y, self.x = (me // 2) % 4, (me // 8) % 2, me // 16
        self.to = {"X": (me + 16) % 32, "Y": (me // 16) * 16 + (me + 8) % 16, "Z": (me // 8) * 8 + (me + 2) % 8}
        self.before = (me // 8) * 8 + (me + 6) % 8
        self.pair = me + 1 - 2 * self.core

    def chip_of(self, rel):
        return ((self.x + rel[0]) % 2) * 8 + ((self.y + rel[1]) % 2) * 4 + (self.z + 4 - rel[2]) % 4

    def piece(self, chip, core, p):
        return self.kv.at[chip * 2 + core, pl.ds(p * 128, 128), :]

    def greet(self):
        barrier = pltpu.get_barrier_semaphore()
        for d in (self.to["X"], self.to["Y"], self.to["Z"], self.before, self.pair):
            pl.semaphore_signal(barrier, inc=1, device_id={"sp": d})

    def greeted(self):
        pl.semaphore_wait(pltpu.get_barrier_semaphore(), 5)

    def link(self, i):
        link, rel, p, _, _ = COPIES[i]
        ref = self.piece(self.chip_of(rel), self.core, p)
        return pltpu.make_async_remote_copy(ref, ref, self.s_link.at[i], self.r_link.at[i], device_id={"sp": self.to[link]})

    def came(self, i):
        link, rel, p, _, _ = COPIES[i]
        ref = self.piece(self.chip_of(_arrives_as(link, rel)), self.core, p)
        return pltpu.make_async_remote_copy(ref, ref, self.s_link.at[i], self.r_link.at[i], device_id={"sp": self.to[link]})

    def across(self, rel, p, core):
        i = (rel[0] * 8 + rel[1] * 4 + rel[2]) * 4 + p
        ref = self.piece(self.chip_of(rel), core, p)
        return pltpu.make_async_remote_copy(ref, ref, self.s_pair.at[i], self.r_pair.at[i], device_id={"sp": self.pair})

    def among(self, bits):
        return lax.rem(lax.shift_right_logical(jnp.int32(bits), self.chip), 2) == 1

    def run(self, slot):
        for _, kind, _, i in slot:
            link, rel, p, _, _ = COPIES[i]
            if kind == 1:
                pl.when(self.among(SENDS[i]))(self.link(i).start)
            else:
                here = _arrives_as(link, rel)
                pl.when(self.among(GETS[i]))(self.came(i).wait_recv)
                pl.when(self.chip_of(here) < self.chip)(self.across(here, p, self.core).start)

    def finish(self):
        for i in range(len(COPIES)):
            pl.when(self.among(SENDS[i]))(self.link(i).wait_send)
        for rel in [(0, 0, 0), *RELS]:
            @pl.when(self.chip_of(rel) <= self.chip)
            def _():
                for p in range(4):
                    self.across(rel, p, self.core).wait_send()


class _Softmax:
    def __init__(self, kv, q_s, top_s, mix_s, open_p, open_keep, open_s):
        self.kv, self.q_s, self.top_s, self.mix_s = kv, q_s, top_s, mix_s
        self.open_p, self.open_keep, self.open_s = open_p, open_keep, open_s

    def keys(self, chip):
        return jnp.concatenate([self.kv[2 * chip + i, 0:256, :] for i in range(2)], axis=0)

    def values(self, chip):
        v = jnp.concatenate([self.kv[2 * chip + i, 256:512, :].T for i in range(2)], axis=1)
        return jnp.concatenate([v, jnp.ones((8, 512), jnp.bfloat16)], axis=0)

    def weights(self, s, h):
        at = slice(h * OWN, (h + 1) * OWN)
        old = self.top_s[0:1, at]
        top = jnp.maximum(old, s.max(axis=0, keepdims=True))
        self.top_s[0:1, at] = top
        return jnp.exp2((s - top) * E).astype(jnp.bfloat16), jnp.exp2((old - top) * E)

    def add(self, h, v, p, keep):
        at = slice(h * OWN, (h + 1) * OWN)
        self.mix_s[:, at] = self.mix_s[:, at] * keep + _dot(v, p, 1, 0)

    def step(self, chip, before=None, visible=None):
        k, v, last = self.keys(chip), self.values(chip), HEADS - 1
        scores, done = {}, {}

        def score(h):
            s = _dot(k, self.q_s[h * OWN : (h + 1) * OWN, :], 1, 1)
            scores[h] = s if visible is None else jnp.where(visible, s, HIDDEN)

        def close(h):
            done[h] = self.weights(scores.pop(h), h)

        if before is not None:
            v_before, s_before = self.values(before), self.open_s[...]
        score(0)
        if before is not None:
            self.add(last - 1, v_before, self.open_p[...], self.open_keep[0:1, :])
            closed = self.weights(s_before, last)
        score(1)
        close(0)
        if before is not None:
            self.add(last, v_before, *closed)
        for h in range(2, HEADS):
            score(h)
            close(h - 1)
            self.add(h - 2, v, *done.pop(h - 2))
        self.open_p[...], self.open_keep[0:1, :] = done.pop(last - 1)
        self.open_s[...] = scores.pop(last)

    def finish(self, before):
        v, last = self.values(before), HEADS - 1
        self.add(last - 1, v, self.open_p[...], self.open_keep[0:1, :])
        self.add(last, v, *self.weights(self.open_s[...], last))


def _kernel(x_h, gain_h, wq_h, wk_h, wv_h, cos_h, sin_h, base_h, seen_ref,
            x_s, gain_s, wq_s, wkv_s, cos_s, sin_s, base_s, a_s, q_s, kv, top_s, mix_s, open_p, open_keep, open_s, in_sem, s_link, r_link, s_pair, r_pair):
    ring = _Ring(kv, s_link, r_link, s_pair, r_pair)
    me = ring.me
    ring.greet()
    first = [(x_h, x_s), (gain_h, gain_s), (wk_h, wkv_s.at[:, pl.ds(0, HEAD)]), (wv_h, wkv_s.at[:, pl.ds(HEAD, HEAD)]),
             (cos_h, cos_s), (sin_h, sin_s), (base_h, base_s)]
    later = [(wq_h.at[:, pl.ds(512 * i, 512)], wq_s.at[:, pl.ds(512 * i, 512)]) for i in range(4)]
    first, later = ([pltpu.make_async_copy(a, b, in_sem.at[n + i]) for i, (a, b) in enumerate(c)] for n, c in ((0, first), (7, later)))
    for c in first:
        c.start()
    for c in first:
        c.wait()
    for c in later[:4]:
        c.start()

    wide = x_s[...].astype(jnp.float32)
    scale = lax.rsqrt(jnp.mean(wide * wide, -1, keepdims=True) + 1e-6)
    a_s[...] = (wide * scale * gain_s[...].astype(jnp.float32)[None]).astype(jnp.bfloat16)
    here = base_s[me]
    cb, sb = here[:, :HALF], here[:, HALF:]
    cos = cb * cos_s[...] - sb * sin_s[...]
    sin = sb * cos_s[...] + cb * sin_s[...]
    cos_s[...] = cos
    sin_s[...] = sin
    both = _dot(a_s[...], wkv_s[...], 1, 0)
    kv[me, 0:256, :] = _turn(both[:, :HEAD], cos, sin)
    kv[me, 256:512, :] = both[:, HEAD:].astype(jnp.bfloat16)

    ring.greeted()
    for p in range(4):
        ring.across((0, 0, 0), p, ring.core).start()
    slots = _slots()
    for i in range(4):
        ring.run(slots[i])
        later[i].wait()
        for h in (2 * i, 2 * i + 1):
            q = _dot(a_s[...], wq_s[:, h * HEAD : (h + 1) * HEAD], 1, 0)
            q_s[h * OWN : (h + 1) * OWN, :] = _turn(q, cos_s[...], sin_s[...])

    ring.run(slots[4])
    top_s[...] = jnp.full(top_s.shape, NEG, jnp.float32)
    mix_s[...] = jnp.zeros(mix_s.shape, jnp.float32)
    for p in range(4):
        ring.across((0, 0, 0), p, 1 - ring.core).wait_recv()
    softmax = _Softmax(kv, q_s, top_s, mix_s, open_p, open_keep, open_s)
    place = ring.core * OWN + lax.broadcasted_iota(jnp.int32, (512, OWN), 1)
    softmax.step(ring.chip, None, place >= lax.broadcasted_iota(jnp.int32, (512, OWN), 0))

    def step(n, before):
        chip = 0
        for i, rel in enumerate(RELS):
            chip = jnp.where(n == i, ring.chip_of(rel), chip)
        for four in range(0, len(RELS), 4):
            @pl.when(n // 4 == four // 4)
            def _():
                for i, rel in list(enumerate(RELS))[four : four + 4]:
                    @pl.when(n == i)
                    def _():
                        ring.run(slots[5 + i])

                        @pl.when(ring.chip_of(rel) < ring.chip)
                        def _():
                            for p in range(4):
                                ring.across(rel, p, 1 - ring.core).wait_recv()

        seen = chip < ring.chip

        @pl.when(seen)
        def _():
            softmax.step(chip, before)

        return jnp.where(seen, chip, before)

    softmax.finish(lax.fori_loop(0, len(RELS), step, ring.chip))
    for h in range(HEADS):
        at = slice(h * OWN, (h + 1) * OWN)
        part = mix_s[:HEAD, at] * (1 / mix_s[HEAD : HEAD + 1, at])
        seen_ref[:, h * HEAD : (h + 1) * HEAD] = part.astype(jnp.bfloat16).T
    ring.finish()


def _tables():
    freq = THETA ** (-np.arange(HALF) / HALF)
    place = np.arange(OWN)[:, None] * freq
    start = (np.arange(DEVICES) * OWN)[:, None] * freq
    base = np.concatenate([np.cos(start), np.sin(start)], axis=1)[:, None]
    return [jnp.asarray(t, jnp.float32) for t in (np.cos(place), np.sin(place), base)]


def _out(x_ref, seen_ref, wo_ref, y_ref, y_s, sem):
    copies = []
    for i in range(4):
        at = slice(512 * i, 512 * (i + 1))
        y = _dot(seen_ref[...], wo_ref[:, at], 1, 0)
        y_s[:, at] = (x_ref[:, at].astype(jnp.float32) + y).astype(jnp.bfloat16)
        copies.append(pltpu.make_async_copy(y_s.at[:, pl.ds(512 * i, 512)], y_ref.at[:, pl.ds(512 * i, 512)], sem.at[i]))
        copies[-1].start()
    for c in copies:
        c.wait()


def _project(x, seen, wo):
    return pl.pallas_call(
        _out,
        out_shape=jax.ShapeDtypeStruct((OWN, D), jnp.bfloat16),
        in_specs=[pl.BlockSpec(memory_space=pltpu.VMEM)] * 3,
        out_specs=pl.BlockSpec(memory_space=pl.ANY),
        scratch_shapes=[pltpu.VMEM((OWN, D), jnp.bfloat16), pltpu.SemaphoreType.DMA((4,))],
        compiler_params=pltpu.CompilerParams(vmem_limit_bytes=24 * 2**20),
        name="project",
    )(x, seen, wo)


def solution(mesh):
    def step(x, gain, wq, wk, wv, wo):
        vmem = lambda *shape: pltpu.VMEM(shape, jnp.bfloat16)
        wide = lambda *shape: pltpu.VMEM(shape, jnp.float32)
        dma = pltpu.SemaphoreType.DMA
        seen = pl.pallas_call(
            _kernel,
            out_shape=jax.ShapeDtypeStruct((OWN, D), jnp.bfloat16),
            in_specs=[pl.BlockSpec(memory_space=pl.ANY)] * 8,
            out_specs=pl.BlockSpec(memory_space=pltpu.VMEM),
            scratch_shapes=[vmem(OWN, D), vmem(D), vmem(D, D), vmem(D, 2 * HEAD), wide(OWN, HALF), wide(OWN, HALF),
                            wide(DEVICES, 1, HEAD), vmem(OWN, D), vmem(COLS, HEAD), vmem(DEVICES, 2 * OWN, HEAD),
                            wide(8, COLS), wide(HEAD + 8, COLS), vmem(512, OWN), wide(8, OWN), wide(512, OWN), dma((12,)), dma((len(COPIES),)), dma((len(COPIES),)), dma((64,)), dma((64,))],
            compiler_params=pltpu.CompilerParams(collective_id=0, has_side_effects=True, vmem_limit_bytes=40 * 2**20),
            cost_estimate=pl.CostEstimate(flops=2**34, bytes_accessed=2**24, transcendentals=2**24),
            name="layer",
        )(*(pltpu.with_memory_space_constraint(t, pltpu.HBM) for t in (x, gain, wq, wk, wv, *_tables())))
        return _project(x, seen, wo)

    tokens, whole = P(("dp", "sp"), None), P(None, None)
    return jax.shard_map(step, mesh=mesh, in_specs=(tokens, P(None), whole, whole, whole, whole), out_specs=tokens, check_vma=False)
```

```python
import functools

import jax
import jax.numpy as jnp
import numpy as np
from jax import lax
from jax.experimental import pallas as pl
from jax.experimental.pallas import tpu as pltpu
from jax.sharding import PartitionSpec as P

D = 2048
HEADS = 8
HEAD = 256
HALF = 128
OWN = 256
DEVICES = 32
THETA = 10000
NEG = -1e30
HIDDEN = 2 * NEG
E = HEAD**-0.5 * 1.4426950408889634
COLS = HEADS * OWN

ORDER = {
    "X": (1, 0, 3, 2, 16, 5, 6, 7, 17, 20, 9, 11, 10, 23, 24, 13, 15, 14, 28, 31),
    "Y": (0, 1, 3, 2, 5, 6, 7, 34, 35, 37, 38, 9, 11, 10, 41, 43, 42, 15, 46),
    "Z": (1, 2, 3, 0, 16, 32, 5, 7, 6, 4, 20, 36, 9, 11, 10, 8, 24, 25, 40, 26, 57),
}

LATENCY = {"X": 3.13, "Y": 3.13, "Z": 4.03}


def _arrives_as(link, rel):
    return rel[0] ^ (link == "X"), rel[1] ^ (link == "Y"), (rel[2] + (link == "Z")) % 4


def _planned():
    left = {link: [((n // 32, n // 16 % 2, n // 4 % 4), n % 4) for n in order] for link, order in ORDER.items()}
    free = dict.fromkeys(ORDER, 0.0)
    here = {((0, 0, 0), p): 0.0 for p in range(4)}
    copies = []
    while any(left.values()):
        for link, rest in left.items():
            if rest and rest[0] in here:
                rel, p = rest.pop(0)
                start = max(free[link], here[rel, p])
                free[link] = start + 1
                here[_arrives_as(link, rel), p] = start + 1 + LATENCY[link]
                copies.append((link, rel, p, start, start + 1 + LATENCY[link]))
    return sorted(copies, key=lambda c: c[3])


COPIES = _planned()


def _events():
    events, came = [], {}
    for i, (link, rel, p, start, arrive) in enumerate(COPIES):
        came[_arrives_as(link, rel), p] = (arrive, i)
    for i, (link, rel, p, start, arrive) in enumerate(COPIES):
        ready = came[rel, p][0] if (rel, p) in came else 0.0
        events.append((max(ready, start - AHEAD), 1, start, i))
    for (rel, p), (arrive, i) in came.items():
        onward = any(c[1:3] == (rel, p) for c in COPIES)
        events.append((arrive if onward else arrive + LATE, 0, arrive, i))
    return sorted(events), came


def _from(chip, rel):
    return (chip // 8 + rel[0]) % 2 * 8 + (chip // 4 + rel[1]) % 2 * 4 + (chip + 4 - rel[2]) % 4


def _next(chip, link):
    step = {"X": (1, 0, 0), "Y": (0, 1, 0), "Z": (0, 0, 3)}[link]
    return _from(chip, step)


def _used():
    @functools.cache
    def used(chip, i):
        link, rel, p, _, _ = COPIES[i]
        to, came = _next(chip, link), _arrives_as(link, rel)
        on = [j for j, c in enumerate(COPIES) if c[1:3] == (came, p)]
        return _from(chip, rel) < to or any(used(to, j) for j in on)

    sends, gets = [0] * len(COPIES), [0] * len(COPIES)
    for i, copy in enumerate(COPIES):
        for chip in range(16):
            if used(chip, i):
                sends[i] |= 1 << chip
                gets[i] |= 1 << _next(chip, copy[0])
    return sends, gets


SENDS, GETS = _used()
AHEAD = 1
LATE = 1
EVENTS, CAME = _events()
RELS = sorted({rel for rel, _ in CAME}, key=lambda rel: (max(CAME[rel, p][0] for p in range(4)), rel))
T_QUERIES, T_FIRST, T_STEP = 0.5, 2.42, 1.17


def _slots():
    times = [T_QUERIES * i for i in range(4)] + [T_FIRST + T_STEP * i for i in range(len(RELS))]
    slots, at, got = [], 0, set()
    for n, t in enumerate(times):
        slot = []
        need = {CAME[RELS[n - 4], p][1] for p in range(4)} if n >= 4 else set()
        while at < len(EVENTS) and (EVENTS[at][0] <= t or not need <= got):
            slot.append(EVENTS[at])
            if EVENTS[at][1] == 0:
                got.add(EVENTS[at][3])
            at += 1
        slots.append(slot)
    return slots + [EVENTS[at:]]


def _dot(a, b, ca, cb):
    return lax.dot_general(a, b, (((ca,), (cb,)), ((), ())), preferred_element_type=jnp.float32)


def _turn(t, cos, sin):
    t = t.astype(jnp.bfloat16).astype(jnp.float32)
    a, b = t[:, :HALF], t[:, HALF:]
    return jnp.concatenate([a * cos - b * sin, b * cos + a * sin], axis=1).astype(jnp.bfloat16)


def _send_slots():
    order = {axis: [i for _, kind, _, i in EVENTS if kind == 1 and COPIES[i][0] == axis] for axis in ORDER}
    slot, had = {}, {}
    for n, copies in enumerate(order.values()):
        for k, i in enumerate(copies):
            slot[i] = n * RING + k % RING
            had[i] = copies[k - RING] if k >= RING else None
    return slot, had


RING = 6
SLOT, HAD = _send_slots()


class _Ring:
    def __init__(self, kv, s_link, r_link, s_pair, r_pair):
        self.kv, self.s_link, self.r_link, self.s_pair, self.r_pair = kv, s_link, r_link, s_pair, r_pair
        me = lax.axis_index("sp")
        self.me, self.chip, self.core = me, me // 2, me % 2
        self.z, self.y, self.x = (me // 2) % 4, (me // 8) % 2, me // 16
        self.to = {"X": (me + 16) % 32, "Y": (me // 16) * 16 + (me + 8) % 16, "Z": (me // 8) * 8 + (me + 2) % 8}
        self.before = (me // 8) * 8 + (me + 6) % 8
        self.pair = me + 1 - 2 * self.core

    def chip_of(self, rel):
        return ((self.x + rel[0]) % 2) * 8 + ((self.y + rel[1]) % 2) * 4 + (self.z + 4 - rel[2]) % 4

    def piece(self, chip, core, p):
        return self.kv.at[chip * 2 + core, pl.ds(p * 128, 128), :]

    def greet(self):
        barrier = pltpu.get_barrier_semaphore()
        for d in (self.to["X"], self.to["Y"], self.to["Z"], self.before, self.pair):
            pl.semaphore_signal(barrier, inc=1, device_id={"sp": d})

    def greeted(self):
        pl.semaphore_wait(pltpu.get_barrier_semaphore(), 5)

    def link(self, i):
        link, rel, p, _, _ = COPIES[i]
        ref = self.piece(self.chip_of(rel), self.core, p)
        return pltpu.make_async_remote_copy(ref, ref, self.s_link.at[SLOT[i]], self.r_link.at[i], device_id={"sp": self.to[link]})

    def came(self, i):
        link, rel, p, _, _ = COPIES[i]
        ref = self.piece(self.chip_of(_arrives_as(link, rel)), self.core, p)
        return pltpu.make_async_remote_copy(ref, ref, self.s_link.at[SLOT[i]], self.r_link.at[i], device_id={"sp": self.to[link]})

    def across(self, rel, p, core):
        i, chip = rel[0] * 8 + rel[1] * 4 + rel[2], self.chip_of(rel)
        if p is None:
            return self.block(chip, i, core)
        ref = self.piece(chip, core, p)
        return pltpu.make_async_remote_copy(ref, ref, self.s_pair.at[i], self.r_pair.at[i], device_id={"sp": self.pair})

    def block(self, chip, i, core):
        ref = self.kv.at[chip * 2 + core]
        return pltpu.make_async_remote_copy(ref, ref, self.s_pair.at[i], self.r_pair.at[i], device_id={"sp": self.pair})

    def among(self, bits):
        return lax.rem(lax.shift_right_logical(jnp.int32(bits), self.chip), 2) == 1

    def run(self, slot):
        for _, kind, _, i in slot:
            link, rel, p, _, _ = COPIES[i]
            if kind == 1:
                if HAD[i] is not None:
                    pl.when(self.among(SENDS[HAD[i]]))(self.link(HAD[i]).wait_send)
                pl.when(self.among(SENDS[i]))(self.link(i).start)
            else:
                here = _arrives_as(link, rel)
                pl.when(self.among(GETS[i]))(self.came(i).wait_recv)
                pl.when(self.chip_of(here) < self.chip)(self.across(here, p, self.core).start)

    def finish(self):
        for i in sorted(set(SLOT) - set(HAD.values())):
            pl.when(self.among(SENDS[i]))(self.link(i).wait_send)
        for rel in [(0, 0, 0), *RELS]:
            pl.when(self.chip_of(rel) <= self.chip)(self.across(rel, None, self.core).wait_send)


class _Softmax:
    def __init__(self, kv, q_s, top_s, mix_s, open_p, open_keep, open_s):
        self.kv, self.q_s, self.top_s, self.mix_s = kv, q_s, top_s, mix_s
        self.open_p, self.open_keep, self.open_s = open_p, open_keep, open_s

    def keys(self, chip):
        return jnp.concatenate([self.kv[2 * chip + i, 0:256, :] for i in range(2)], axis=0)

    def values(self, chip):
        v = jnp.concatenate([self.kv[2 * chip + i, 256:512, :].T for i in range(2)], axis=1)
        return jnp.concatenate([v, jnp.ones((8, 512), jnp.bfloat16)], axis=0)

    def weights(self, s, h):
        at = slice(h * OWN, (h + 1) * OWN)
        old = self.top_s[0:1, at]
        top = jnp.maximum(old, s.max(axis=0, keepdims=True))
        self.top_s[0:1, at] = top
        return jnp.exp2((s - top) * E).astype(jnp.bfloat16), jnp.exp2((old - top) * E)

    def add(self, h, v, p, keep):
        at = slice(h * OWN, (h + 1) * OWN)
        self.mix_s[:, at] = self.mix_s[:, at] * keep + _dot(v, p, 1, 0)

    def step(self, chip, before=None, visible=None):
        k, v, last = self.keys(chip), self.values(chip), HEADS - 1
        scores, done = {}, {}

        def score(h):
            s = _dot(k, self.q_s[h * OWN : (h + 1) * OWN, :], 1, 1)
            scores[h] = s if visible is None else jnp.where(visible, s, HIDDEN)

        def close(h):
            done[h] = self.weights(scores.pop(h), h)

        if before is not None:
            v_before, s_before = self.values(before), self.open_s[...]
        score(0)
        if before is not None:
            self.add(last - 1, v_before, self.open_p[...], self.open_keep[0:1, :])
            closed = self.weights(s_before, last)
        score(1)
        close(0)
        if before is not None:
            self.add(last, v_before, *closed)
        for h in range(2, HEADS):
            score(h)
            close(h - 1)
            self.add(h - 2, v, *done.pop(h - 2))
        self.open_p[...], self.open_keep[0:1, :] = done.pop(last - 1)
        self.open_s[...] = scores.pop(last)

    def finish(self, before):
        v, last = self.values(before), HEADS - 1
        self.add(last - 1, v, self.open_p[...], self.open_keep[0:1, :])
        self.add(last, v, *self.weights(self.open_s[...], last))


def _kernel(x_h, gain_h, wq_h, wk_h, wv_h, wo_h, cos_h, sin_h, base_h, seen_ref, wo_ref, x_s,
            gain_s, wq_s, wkv_s, cos_s, sin_s, base_s, a_s, q_s, kv, top_s, mix_s, open_p, open_keep, open_s, in_sem, s_link, r_link, s_pair, r_pair):
    ring = _Ring(kv, s_link, r_link, s_pair, r_pair)
    me = ring.me
    ring.greet()
    first = [(x_h, x_s), (gain_h, gain_s), (cos_h, cos_s), (sin_h, sin_s), (base_h, base_s),
             (wk_h, wkv_s.at[:, pl.ds(0, HEAD)]), (wv_h, wkv_s.at[:, pl.ds(HEAD, HEAD)])]
    later = [(wq_h.at[:, pl.ds(512 * i, 512)], wq_s.at[:, pl.ds(512 * i, 512)]) for i in range(4)] + [(wo_h, wo_ref)]
    first, later = ([pltpu.make_async_copy(a, b, in_sem.at[n + i]) for i, (a, b) in enumerate(c)] for n, c in ((0, first), (7, later)))
    for c in first:
        c.start()
    for c in first[:5]:
        c.wait()

    wide = x_s[...].astype(jnp.float32)
    scale = lax.rsqrt(jnp.mean(wide * wide, -1, keepdims=True) + 1e-6)
    a_s[...] = (wide * scale * gain_s[...].astype(jnp.float32)[None]).astype(jnp.bfloat16)
    here = base_s[me]
    cb, sb = here[:, :HALF], here[:, HALF:]
    cos = cb * cos_s[...] - sb * sin_s[...]
    sin = sb * cos_s[...] + cb * sin_s[...]
    cos_s[...] = cos
    sin_s[...] = sin
    for c in first[5:]:
        c.wait()
    for c in later[:2]:
        c.start()
    both = _dot(a_s[...], wkv_s[...], 1, 0)
    kv[me, 0:256, :] = _turn(both[:, :HEAD], cos, sin)
    kv[me, 256:512, :] = both[:, HEAD:].astype(jnp.bfloat16)

    ring.greeted()
    slots = _slots()
    for i in range(4):
        ring.run(slots[i])
        if i == 0:
            for p in range(4):
                ring.across((0, 0, 0), p, ring.core).start()
            for c in later[2:]:
                c.start()
        later[i].wait()
        for h in (2 * i, 2 * i + 1):
            q = _dot(a_s[...], wq_s[:, h * HEAD : (h + 1) * HEAD], 1, 0)
            q_s[h * OWN : (h + 1) * OWN, :] = _turn(q, cos_s[...], sin_s[...])

    ring.run(slots[4])
    top_s[...] = jnp.full(top_s.shape, NEG, jnp.float32)
    mix_s[...] = jnp.zeros(mix_s.shape, jnp.float32)
    ring.across((0, 0, 0), None, 1 - ring.core).wait_recv()
    softmax = _Softmax(kv, q_s, top_s, mix_s, open_p, open_keep, open_s)
    place = ring.core * OWN + lax.broadcasted_iota(jnp.int32, (512, OWN), 1)
    softmax.step(ring.chip, None, place >= lax.broadcasted_iota(jnp.int32, (512, OWN), 0))

    def step(n, before):
        chip = place = 0
        for i, rel in enumerate(RELS):
            chip = jnp.where(n == i, ring.chip_of(rel), chip)
            place = jnp.where(n == i, rel[0] * 8 + rel[1] * 4 + rel[2], place)
        for four in range(0, len(RELS), 4):
            @pl.when(n // 4 == four // 4)
            def _():
                for i in range(four, min(four + 4, len(RELS))):
                    if slots[5 + i]:
                        @pl.when(n == i)
                        def _():
                            ring.run(slots[5 + i])

        seen = chip < ring.chip

        @pl.when(seen)
        def _():
            ring.block(chip, place, 1 - ring.core).wait_recv()
            softmax.step(chip, before)

        return jnp.where(seen, chip, before)

    softmax.finish(lax.fori_loop(0, len(RELS), step, ring.chip))
    for h in range(HEADS):
        at = slice(h * OWN, (h + 1) * OWN)
        part = mix_s[:HEAD, at] * (1 / mix_s[HEAD : HEAD + 1, at])
        seen_ref[:, h * HEAD : (h + 1) * HEAD] = part.astype(jnp.bfloat16).T
    ring.finish()
    later[4].wait()


def _tables():
    freq = THETA ** (-np.arange(HALF) / HALF)
    place = np.arange(OWN)[:, None] * freq
    start = (np.arange(DEVICES) * OWN)[:, None] * freq
    base = np.concatenate([np.cos(start), np.sin(start)], axis=1)[:, None]
    return [jnp.asarray(t, jnp.float32) for t in (np.cos(place), np.sin(place), base)]


def _out(x_ref, seen_ref, wo_ref, y_ref, y_s, sem):
    copies = []
    for i in range(4):
        at = slice(512 * i, 512 * (i + 1))
        y = _dot(seen_ref[...], wo_ref[:, at], 1, 0)
        y_s[:, at] = (x_ref[:, at].astype(jnp.float32) + y).astype(jnp.bfloat16)
        copies.append(pltpu.make_async_copy(y_s.at[:, pl.ds(512 * i, 512)], y_ref.at[:, pl.ds(512 * i, 512)], sem.at[i]))
        copies[-1].start()
    for c in copies:
        c.wait()


def _project(x, seen, wo):
    return pl.pallas_call(
        _out,
        out_shape=jax.ShapeDtypeStruct((OWN, D), jnp.bfloat16),
        in_specs=[pl.BlockSpec(memory_space=pltpu.VMEM)] * 3,
        out_specs=pl.BlockSpec(memory_space=pl.ANY),
        scratch_shapes=[pltpu.VMEM((OWN, D), jnp.bfloat16), pltpu.SemaphoreType.DMA((4,))],
        compiler_params=pltpu.CompilerParams(vmem_limit_bytes=24 * 2**20),
        name="project",
    )(x, seen, wo)


def solution(mesh):
    def step(x, gain, wq, wk, wv, wo):
        vmem = lambda *shape: pltpu.VMEM(shape, jnp.bfloat16)
        wide = lambda *shape: pltpu.VMEM(shape, jnp.float32)
        dma = pltpu.SemaphoreType.DMA
        seen, wo, x = pl.pallas_call(
            _kernel,
            out_shape=[jax.ShapeDtypeStruct((n, D), jnp.bfloat16) for n in (OWN, D, OWN)],
            in_specs=[pl.BlockSpec(memory_space=pl.ANY)] * 9,
            out_specs=[pl.BlockSpec(memory_space=pltpu.VMEM)] * 3,
            scratch_shapes=[vmem(D), vmem(D, D), vmem(D, 2 * HEAD), wide(OWN, HALF), wide(OWN, HALF),
                            wide(DEVICES, 1, HEAD), vmem(OWN, D), vmem(COLS, HEAD), vmem(DEVICES, 2 * OWN, HEAD),
                            wide(8, COLS), wide(HEAD + 8, COLS), vmem(512, OWN), wide(8, OWN), wide(512, OWN), dma((12,)), dma((3 * RING,)), dma((len(COPIES),)), dma((16,)), dma((16,))],
            compiler_params=pltpu.CompilerParams(collective_id=0, has_side_effects=True, vmem_limit_bytes=40 * 2**20),
            cost_estimate=pl.CostEstimate(flops=2**34, bytes_accessed=2**24, transcendentals=2**24),
            name="layer",
        )(*(pltpu.with_memory_space_constraint(t, pltpu.HBM) for t in (x, gain, wq, wk, wv, wo, *_tables())))
        return _project(x, seen, wo)

    tokens, whole = P(("dp", "sp"), None), P(None, None)
    return jax.shard_map(step, mesh=mesh, in_specs=(tokens, P(None), whole, whole, whole, whole), out_specs=tokens, check_vma=False)
```

```python
import functools

import jax
import jax.numpy as jnp
import numpy as np
from jax import lax
from jax.experimental import pallas as pl
from jax.experimental.pallas import tpu as pltpu
from jax.sharding import PartitionSpec as P

D = 2048
HEADS = 8
HEAD = 256
HALF = 128
OWN = 256
DEVICES = 32
THETA = 10000
NEG = -1e30
HIDDEN = 2 * NEG
E = HEAD**-0.5 * 1.4426950408889634
COLS = HEADS * OWN

ORDER = {
    "X": (1, 0, 3, 2, 16, 5, 6, 7, 17, 20, 9, 11, 10, 23, 24, 13, 15, 14, 28, 31),
    "Y": (0, 1, 3, 2, 5, 6, 7, 34, 35, 37, 38, 9, 11, 10, 41, 43, 42, 15, 46),
    "Z": (1, 2, 3, 0, 16, 32, 5, 7, 6, 4, 20, 36, 9, 11, 10, 8, 24, 25, 40, 26, 57),
}

LATENCY = {"X": 3.13, "Y": 3.13, "Z": 4.03}


def _arrives_as(link, rel):
    return rel[0] ^ (link == "X"), rel[1] ^ (link == "Y"), (rel[2] + (link == "Z")) % 4


def _planned():
    left = {link: [((n // 32, n // 16 % 2, n // 4 % 4), n % 4) for n in order] for link, order in ORDER.items()}
    free = dict.fromkeys(ORDER, 0.0)
    here = {((0, 0, 0), p): 0.0 for p in range(4)}
    copies = []
    while any(left.values()):
        for link, rest in left.items():
            if rest and rest[0] in here:
                rel, p = rest.pop(0)
                start = max(free[link], here[rel, p])
                free[link] = start + 1
                here[_arrives_as(link, rel), p] = start + 1 + LATENCY[link]
                copies.append((link, rel, p, start, start + 1 + LATENCY[link]))
    return sorted(copies, key=lambda c: c[3])


COPIES = _planned()


def _events():
    events, came = [], {}
    for i, (link, rel, p, start, arrive) in enumerate(COPIES):
        came[_arrives_as(link, rel), p] = (arrive, i)
    for i, (link, rel, p, start, arrive) in enumerate(COPIES):
        ready = came[rel, p][0] if (rel, p) in came else 0.0
        events.append((max(ready, start - AHEAD), 1, start, i))
    for (rel, p), (arrive, i) in came.items():
        onward = any(c[1:3] == (rel, p) for c in COPIES)
        events.append((arrive if onward else arrive + LATE, 0, arrive, i))
    return sorted(events), came


def _from(chip, rel):
    return (chip // 8 + rel[0]) % 2 * 8 + (chip // 4 + rel[1]) % 2 * 4 + (chip + 4 - rel[2]) % 4


def _next(chip, link):
    step = {"X": (1, 0, 0), "Y": (0, 1, 0), "Z": (0, 0, 3)}[link]
    return _from(chip, step)


def _used():
    @functools.cache
    def used(chip, i):
        link, rel, p, _, _ = COPIES[i]
        to, came = _next(chip, link), _arrives_as(link, rel)
        on = [j for j, c in enumerate(COPIES) if c[1:3] == (came, p)]
        return _from(chip, rel) < to or any(used(to, j) for j in on)

    sends, gets = [0] * len(COPIES), [0] * len(COPIES)
    for i, copy in enumerate(COPIES):
        for chip in range(16):
            if used(chip, i):
                sends[i] |= 1 << chip
                gets[i] |= 1 << _next(chip, copy[0])
    return sends, gets


SENDS, GETS = _used()
AHEAD = 1
LATE = 1
EVENTS, CAME = _events()
RELS = sorted({rel for rel, _ in CAME}, key=lambda rel: (max(CAME[rel, p][0] for p in range(4)), rel))
T_QUERIES, T_FIRST, T_STEP = 0.5, 2.42, 1.17


def _slots():
    times = [T_QUERIES * i for i in range(4)] + [T_FIRST + T_STEP * i for i in range(len(RELS))]
    slots, at, got = [], 0, set()
    for n, t in enumerate(times):
        slot = []
        need = {CAME[RELS[n - 4], p][1] for p in range(4)} if n >= 4 else set()
        while at < len(EVENTS) and (EVENTS[at][0] <= t or not need <= got):
            slot.append(EVENTS[at])
            if EVENTS[at][1] == 0:
                got.add(EVENTS[at][3])
            at += 1
        slots.append(slot)
    return slots + [EVENTS[at:]]


def _dot(a, b, ca, cb):
    return lax.dot_general(a, b, (((ca,), (cb,)), ((), ())), preferred_element_type=jnp.float32)


def _turn(t, cos, sin):
    t = t.astype(jnp.bfloat16).astype(jnp.float32)
    a, b = t[:, :HALF], t[:, HALF:]
    return jnp.concatenate([a * cos - b * sin, b * cos + a * sin], axis=1).astype(jnp.bfloat16)


def _send_slots():
    order = {axis: [i for _, kind, _, i in EVENTS if kind == 1 and COPIES[i][0] == axis] for axis in ORDER}
    slot, had = {}, {}
    for n, copies in enumerate(order.values()):
        for k, i in enumerate(copies):
            slot[i] = n * RING + k % RING
            had[i] = copies[k - RING] if k >= RING else None
    return slot, had


RING = 9
SLOT, HAD = _send_slots()


class _Ring:
    def __init__(self, kv, s_link, r_link, s_pair, r_pair):
        self.kv, self.s_link, self.r_link, self.s_pair, self.r_pair = kv, s_link, r_link, s_pair, r_pair
        me = lax.axis_index("sp")
        self.me, self.chip, self.core = me, me // 2, me % 2
        self.z, self.y, self.x = (me // 2) % 4, (me // 8) % 2, me // 16
        self.to = {"X": (me + 16) % 32, "Y": (me // 16) * 16 + (me + 8) % 16, "Z": (me // 8) * 8 + (me + 2) % 8}
        self.before = (me // 8) * 8 + (me + 6) % 8
        self.pair = me + 1 - 2 * self.core
        places = [(n // 8, n // 4 % 2, n % 4) for n in range(16)]
        self.chips = {r: ((self.x + r[0]) % 2) * 8 + ((self.y + r[1]) % 2) * 4 + (self.z + 4 - r[2]) % 4 for r in places}
        self.bit = lax.shift_left(jnp.int32(1), self.chip)

    def chip_of(self, rel):
        return self.chips[rel]

    def piece(self, chip, core, p):
        return self.kv.at[chip * 2 + core, pl.ds(p * 128, 128), :]

    def greet(self):
        barrier = pltpu.get_barrier_semaphore()
        for d in (self.to["X"], self.to["Y"], self.to["Z"], self.before, self.pair):
            pl.semaphore_signal(barrier, inc=1, device_id={"sp": d})

    def greeted(self):
        pl.semaphore_wait(pltpu.get_barrier_semaphore(), 5)

    def link(self, i):
        link, rel, p, _, _ = COPIES[i]
        ref = self.piece(self.chip_of(rel), self.core, p)
        return pltpu.make_async_remote_copy(ref, ref, self.s_link.at[SLOT[i]], self.r_link.at[i], device_id={"sp": self.to[link]})

    def came(self, i):
        link, rel, p, _, _ = COPIES[i]
        ref = self.piece(self.chip_of(_arrives_as(link, rel)), self.core, p)
        return pltpu.make_async_remote_copy(ref, ref, self.s_link.at[SLOT[i]], self.r_link.at[i], device_id={"sp": self.to[link]})

    def across(self, rel, p, core):
        i, chip = rel[0] * 8 + rel[1] * 4 + rel[2], self.chip_of(rel)
        if p is None:
            return self.block(chip, i, core)
        ref = self.piece(chip, core, p)
        return pltpu.make_async_remote_copy(ref, ref, self.s_pair.at[i], self.r_pair.at[i], device_id={"sp": self.pair})

    def block(self, chip, i, core):
        ref = self.kv.at[chip * 2 + core]
        return pltpu.make_async_remote_copy(ref, ref, self.s_pair.at[i], self.r_pair.at[i], device_id={"sp": self.pair})

    def among(self, bits):
        return (jnp.int32(bits) & self.bit) != 0

    def run(self, slot):
        for _, kind, _, i in slot:
            link, rel, p, _, _ = COPIES[i]
            if kind == 1:
                if HAD[i] is not None:
                    pl.when(self.among(SENDS[HAD[i]]))(self.link(HAD[i]).wait_send)
                pl.when(self.among(SENDS[i]))(self.link(i).start)
            else:
                here = _arrives_as(link, rel)
                pl.when(self.among(GETS[i]))(self.came(i).wait_recv)
                pl.when(self.chip_of(here) < self.chip)(self.across(here, p, self.core).start)

    def finish(self):
        for i in sorted(set(SLOT) - set(HAD.values())):
            pl.when(self.among(SENDS[i]))(self.link(i).wait_send)
        for rel in [(0, 0, 0), *RELS]:
            pl.when(self.chip_of(rel) <= self.chip)(self.across(rel, None, self.core).wait_send)


class _Softmax:
    def __init__(self, kv, q_s, top_s, mix_s, open_p, open_keep, open_s):
        self.kv, self.q_s, self.top_s, self.mix_s = kv, q_s, top_s, mix_s
        self.open_p, self.open_keep, self.open_s = open_p, open_keep, open_s

    def keys(self, chip):
        return jnp.concatenate([self.kv[2 * chip + i, 0:256, :] for i in range(2)], axis=0)

    def values(self, chip):
        v = jnp.concatenate([self.kv[2 * chip + i, 256:512, :].T for i in range(2)], axis=1)
        return jnp.concatenate([v, jnp.ones((8, 512), jnp.bfloat16)], axis=0)

    def weights(self, s, h):
        at = slice(h * OWN, (h + 1) * OWN)
        old = self.top_s[0:1, at]
        top = jnp.maximum(old, s.max(axis=0, keepdims=True))
        self.top_s[0:1, at] = top
        return jnp.exp2((s - top) * E).astype(jnp.bfloat16), jnp.exp2((old - top) * E)

    def add(self, h, v, p, keep):
        at = slice(h * OWN, (h + 1) * OWN)
        self.mix_s[:, at] = self.mix_s[:, at] * keep + _dot(v, p, 1, 0)

    def step(self, chip, before=None, visible=None):
        k, v, last = self.keys(chip), self.values(chip), HEADS - 1
        scores, done = {}, {}

        def score(h):
            s = _dot(k, self.q_s[h * OWN : (h + 1) * OWN, :], 1, 1)
            scores[h] = s if visible is None else jnp.where(visible, s, HIDDEN)

        def close(h):
            done[h] = self.weights(scores.pop(h), h)

        if before is not None:
            v_before, s_before = self.values(before), self.open_s[...]
        score(0)
        if before is not None:
            self.add(last - 1, v_before, self.open_p[...], self.open_keep[0:1, :])
            closed = self.weights(s_before, last)
        score(1)
        close(0)
        if before is not None:
            self.add(last, v_before, *closed)
        for h in range(2, HEADS):
            score(h)
            close(h - 1)
            self.add(h - 2, v, *done.pop(h - 2))
        self.open_p[...], self.open_keep[0:1, :] = done.pop(last - 1)
        self.open_s[...] = scores.pop(last)

    def finish(self, before):
        v, last = self.values(before), HEADS - 1
        self.add(last - 1, v, self.open_p[...], self.open_keep[0:1, :])
        self.add(last, v, *self.weights(self.open_s[...], last))


def _kernel(x_h, gain_h, wq_h, wk_h, wv_h, wo_h, cos_h, sin_h, base_h, seen_ref, wo_ref, x_s,
            gain_s, wq_s, wkv_s, cos_s, sin_s, base_s, a_s, q_s, kv, top_s, mix_s, open_p, open_keep, open_s, in_sem, s_link, r_link, s_pair, r_pair):
    ring = _Ring(kv, s_link, r_link, s_pair, r_pair)
    me = ring.me
    ring.greet()
    first = [(x_h, x_s), (gain_h, gain_s), (cos_h, cos_s), (sin_h, sin_s), (base_h, base_s),
             (wk_h, wkv_s.at[:, pl.ds(0, HEAD)]), (wv_h, wkv_s.at[:, pl.ds(HEAD, HEAD)])]
    later = [(wq_h.at[:, pl.ds(512 * i, 512)], wq_s.at[:, pl.ds(512 * i, 512)]) for i in range(4)] + [(wo_h, wo_ref)]
    first, later = ([pltpu.make_async_copy(a, b, in_sem.at[n + i]) for i, (a, b) in enumerate(c)] for n, c in ((0, first), (7, later)))
    for c in first:
        c.start()
    for c in first[:5]:
        c.wait()

    wide = x_s[...].astype(jnp.float32)
    scale = lax.rsqrt(jnp.mean(wide * wide, -1, keepdims=True) + 1e-6)
    a_s[...] = (wide * scale * gain_s[...].astype(jnp.float32)[None]).astype(jnp.bfloat16)
    here = base_s[me]
    cb, sb = here[:, :HALF], here[:, HALF:]
    cos = cb * cos_s[...] - sb * sin_s[...]
    sin = sb * cos_s[...] + cb * sin_s[...]
    cos_s[...] = cos
    sin_s[...] = sin
    for c in first[5:]:
        c.wait()
    for c in later[:2]:
        c.start()
    both = _dot(a_s[...], wkv_s[...], 1, 0)
    kv[me, 0:256, :] = _turn(both[:, :HEAD], cos, sin)
    kv[me, 256:512, :] = both[:, HEAD:].astype(jnp.bfloat16)

    ring.greeted()
    slots = _slots()
    for i in range(4):
        ring.run(slots[i])
        if i == 0:
            for p in range(4):
                ring.across((0, 0, 0), p, ring.core).start()
            for c in later[2:]:
                c.start()
        later[i].wait()
        for h in (2 * i, 2 * i + 1):
            q = _dot(a_s[...], wq_s[:, h * HEAD : (h + 1) * HEAD], 1, 0)
            q_s[h * OWN : (h + 1) * OWN, :] = _turn(q, cos_s[...], sin_s[...])

    ring.run(slots[4])
    top_s[...] = jnp.full(top_s.shape, NEG, jnp.float32)
    mix_s[...] = jnp.zeros(mix_s.shape, jnp.float32)
    ring.across((0, 0, 0), None, 1 - ring.core).wait_recv()
    softmax = _Softmax(kv, q_s, top_s, mix_s, open_p, open_keep, open_s)
    place = ring.core * OWN + lax.broadcasted_iota(jnp.int32, (512, OWN), 1)
    softmax.step(ring.chip, None, place >= lax.broadcasted_iota(jnp.int32, (512, OWN), 0))

    def step(n, before):
        chip = place = 0
        for i, rel in enumerate(RELS):
            chip = jnp.where(n == i, ring.chip_of(rel), chip)
            place = jnp.where(n == i, rel[0] * 8 + rel[1] * 4 + rel[2], place)
        for four in range(0, len(RELS), 4):
            @pl.when(n // 4 == four // 4)
            def _():
                for i in range(four, min(four + 4, len(RELS))):
                    if slots[5 + i]:
                        @pl.when(n == i)
                        def _():
                            ring.run(slots[5 + i])

        seen = chip < ring.chip

        @pl.when(seen)
        def _():
            ring.block(chip, place, 1 - ring.core).wait_recv()
            softmax.step(chip, before)

        return jnp.where(seen, chip, before)

    softmax.finish(lax.fori_loop(0, len(RELS), step, ring.chip))
    for h in range(HEADS):
        at = slice(h * OWN, (h + 1) * OWN)
        part = mix_s[:HEAD, at] * (1 / mix_s[HEAD : HEAD + 1, at])
        seen_ref[:, h * HEAD : (h + 1) * HEAD] = part.astype(jnp.bfloat16).T
    ring.finish()
    later[4].wait()


def _tables():
    freq = THETA ** (-np.arange(HALF) / HALF)
    place = np.arange(OWN)[:, None] * freq
    start = (np.arange(DEVICES) * OWN)[:, None] * freq
    base = np.concatenate([np.cos(start), np.sin(start)], axis=1)[:, None]
    return [jnp.asarray(t, jnp.float32) for t in (np.cos(place), np.sin(place), base)]


def _out(x_ref, seen_ref, wo_ref, y_ref, y_s, sem):
    copies = []
    for i in range(4):
        at = slice(512 * i, 512 * (i + 1))
        y = _dot(seen_ref[...], wo_ref[:, at], 1, 0)
        y_s[:, at] = (x_ref[:, at].astype(jnp.float32) + y).astype(jnp.bfloat16)
        copies.append(pltpu.make_async_copy(y_s.at[:, pl.ds(512 * i, 512)], y_ref.at[:, pl.ds(512 * i, 512)], sem.at[i]))
        copies[-1].start()
    for c in copies:
        c.wait()


def _project(x, seen, wo):
    return pl.pallas_call(
        _out,
        out_shape=jax.ShapeDtypeStruct((OWN, D), jnp.bfloat16),
        in_specs=[pl.BlockSpec(memory_space=pltpu.VMEM)] * 3,
        out_specs=pl.BlockSpec(memory_space=pl.ANY),
        scratch_shapes=[pltpu.VMEM((OWN, D), jnp.bfloat16), pltpu.SemaphoreType.DMA((4,))],
        compiler_params=pltpu.CompilerParams(vmem_limit_bytes=24 * 2**20),
        name="project",
    )(x, seen, wo)


def solution(mesh):
    def step(x, gain, wq, wk, wv, wo):
        vmem = lambda *shape: pltpu.VMEM(shape, jnp.bfloat16)
        wide = lambda *shape: pltpu.VMEM(shape, jnp.float32)
        dma = pltpu.SemaphoreType.DMA
        seen, wo, x = pl.pallas_call(
            _kernel,
            out_shape=[jax.ShapeDtypeStruct((n, D), jnp.bfloat16) for n in (OWN, D, OWN)],
            in_specs=[pl.BlockSpec(memory_space=pl.ANY)] * 9,
            out_specs=[pl.BlockSpec(memory_space=pltpu.VMEM)] * 3,
            scratch_shapes=[vmem(D), vmem(D, D), vmem(D, 2 * HEAD), wide(OWN, HALF), wide(OWN, HALF),
                            wide(DEVICES, 1, HEAD), vmem(OWN, D), vmem(COLS, HEAD), vmem(DEVICES, 2 * OWN, HEAD),
                            wide(8, COLS), wide(HEAD + 8, COLS), vmem(512, OWN), wide(8, OWN), wide(512, OWN), dma((12,)), dma((3 * RING,)), dma((len(COPIES),)), dma((16,)), dma((16,))],
            compiler_params=pltpu.CompilerParams(collective_id=0, has_side_effects=True, vmem_limit_bytes=40 * 2**20),
            cost_estimate=pl.CostEstimate(flops=2**34, bytes_accessed=2**24, transcendentals=2**24),
            name="layer",
        )(*(pltpu.with_memory_space_constraint(t, pltpu.HBM) for t in (x, gain, wq, wk, wv, wo, *_tables())))
        return _project(x, seen, wo)

    tokens, whole = P(("dp", "sp"), None), P(None, None)
    return jax.shard_map(step, mesh=mesh, in_specs=(tokens, P(None), whole, whole, whole, whole), out_specs=tokens, check_vma=False)
```

```python
import functools

import jax
import jax.numpy as jnp
import numpy as np
from jax import lax
from jax.experimental import pallas as pl
from jax.experimental.pallas import tpu as pltpu
from jax.sharding import PartitionSpec as P

D = 2048
HEADS = 8
HEAD = 256
HALF = 128
OWN = 256
DEVICES = 32
THETA = 10000
NEG = -1e30
HIDDEN = 2 * NEG
E = HEAD**-0.5 * 1.4426950408889634
COLS = HEADS * OWN

ORDER = {
    "X": (1, 0, 3, 2, 16, 5, 6, 7, 17, 20, 9, 11, 10, 23, 24, 13, 15, 14, 28, 31),
    "Y": (0, 1, 3, 2, 5, 6, 7, 34, 35, 37, 38, 9, 11, 10, 41, 43, 42, 15, 46),
    "Z": (1, 2, 3, 0, 16, 32, 5, 7, 6, 4, 20, 36, 9, 11, 10, 8, 24, 25, 40, 26, 57),
}

LATENCY = {"X": 3.13, "Y": 3.13, "Z": 4.03}


def _arrives_as(link, rel):
    return rel[0] ^ (link == "X"), rel[1] ^ (link == "Y"), (rel[2] + (link == "Z")) % 4


def _planned():
    left = {link: [((n // 32, n // 16 % 2, n // 4 % 4), n % 4) for n in order] for link, order in ORDER.items()}
    free = dict.fromkeys(ORDER, 0.0)
    here = {((0, 0, 0), p): 0.0 for p in range(4)}
    copies = []
    while any(left.values()):
        for link, rest in left.items():
            if rest and rest[0] in here:
                rel, p = rest.pop(0)
                start = max(free[link], here[rel, p])
                free[link] = start + 1
                here[_arrives_as(link, rel), p] = start + 1 + LATENCY[link]
                copies.append((link, rel, p, start, start + 1 + LATENCY[link]))
    return sorted(copies, key=lambda c: c[3])


COPIES = _planned()


def _events():
    events, came = [], {}
    for i, (link, rel, p, start, arrive) in enumerate(COPIES):
        came[_arrives_as(link, rel), p] = (arrive, i)
    for i, (link, rel, p, start, arrive) in enumerate(COPIES):
        ready = came[rel, p][0] if (rel, p) in came else 0.0
        events.append((max(ready, start - AHEAD), 1, start, i))
    for (rel, p), (arrive, i) in came.items():
        onward = any(c[1:3] == (rel, p) for c in COPIES)
        events.append((arrive if onward else arrive + LATE, 0, arrive, i))
    return sorted(events), came


def _from(chip, rel):
    return (chip // 8 + rel[0]) % 2 * 8 + (chip // 4 + rel[1]) % 2 * 4 + (chip + 4 - rel[2]) % 4


def _next(chip, link):
    step = {"X": (1, 0, 0), "Y": (0, 1, 0), "Z": (0, 0, 3)}[link]
    return _from(chip, step)


def _used():
    @functools.cache
    def used(chip, i):
        link, rel, p, _, _ = COPIES[i]
        to, came = _next(chip, link), _arrives_as(link, rel)
        on = [j for j, c in enumerate(COPIES) if c[1:3] == (came, p)]
        return _from(chip, rel) < to or any(used(to, j) for j in on)

    sends, gets = [0] * len(COPIES), [0] * len(COPIES)
    for i, copy in enumerate(COPIES):
        for chip in range(16):
            if used(chip, i):
                sends[i] |= 1 << chip
                gets[i] |= 1 << _next(chip, copy[0])
    return sends, gets


SENDS, GETS = _used()
AHEAD = 1
LATE = 1
EVENTS, CAME = _events()
RELS = sorted({rel for rel, _ in CAME}, key=lambda rel: (max(CAME[rel, p][0] for p in range(4)), rel))
T_QUERIES, T_FIRST, T_STEP = 0.5, 2.42, 1.17


def _slots():
    times = [T_QUERIES * i for i in range(4)] + [T_FIRST + T_STEP * i for i in range(len(RELS))]
    slots, at, got = [], 0, set()
    for n, t in enumerate(times):
        slot = []
        need = {CAME[RELS[n - 4], p][1] for p in range(4)} if n >= 4 else set()
        while at < len(EVENTS) and (EVENTS[at][0] <= t or not need <= got):
            slot.append(EVENTS[at])
            if EVENTS[at][1] == 0:
                got.add(EVENTS[at][3])
            at += 1
        slots.append(slot)
    return slots + [EVENTS[at:]]


def _dot(a, b, ca, cb):
    return lax.dot_general(a, b, (((ca,), (cb,)), ((), ())), preferred_element_type=jnp.float32)


def _turn(t, cos, sin):
    t = t.astype(jnp.bfloat16).astype(jnp.float32)
    a, b = t[:, :HALF], t[:, HALF:]
    return jnp.concatenate([a * cos - b * sin, b * cos + a * sin], axis=1).astype(jnp.bfloat16)


def _send_slots():
    order = {axis: [i for _, kind, _, i in EVENTS if kind == 1 and COPIES[i][0] == axis] for axis in ORDER}
    slot, had = {}, {}
    for n, copies in enumerate(order.values()):
        for k, i in enumerate(copies):
            slot[i] = n * RING + k % RING
            had[i] = copies[k - RING] if k >= RING else None
    return slot, had


RING = 9
SLOT, HAD = _send_slots()


class _Ring:
    def __init__(self, kv, s_link, r_link, s_pair, r_pair):
        self.kv, self.s_link, self.r_link, self.s_pair, self.r_pair = kv, s_link, r_link, s_pair, r_pair
        me = lax.axis_index("sp")
        self.me, self.chip, self.core = me, me // 2, me % 2
        self.z, self.y, self.x = (me // 2) % 4, (me // 8) % 2, me // 16
        self.to = {"X": (me + 16) % 32, "Y": (me // 16) * 16 + (me + 8) % 16, "Z": (me // 8) * 8 + (me + 2) % 8}
        self.before = (me // 8) * 8 + (me + 6) % 8
        self.pair = me + 1 - 2 * self.core
        places = [(n // 8, n // 4 % 2, n % 4) for n in range(16)]
        self.chips = {r: ((self.x + r[0]) % 2) * 8 + ((self.y + r[1]) % 2) * 4 + (self.z + 4 - r[2]) % 4 for r in places}
        self.bit = lax.shift_left(jnp.int32(1), self.chip)

    def chip_of(self, rel):
        return self.chips[rel]

    def piece(self, chip, core, p):
        return self.kv.at[chip * 2 + core, pl.ds(p * 128, 128), :]

    def greet(self):
        barrier = pltpu.get_barrier_semaphore()
        for d in (self.to["X"], self.to["Y"], self.to["Z"], self.before, self.pair):
            pl.semaphore_signal(barrier, inc=1, device_id={"sp": d})

    def greeted(self):
        pl.semaphore_wait(pltpu.get_barrier_semaphore(), 5)

    def link(self, i):
        link, rel, p, _, _ = COPIES[i]
        ref = self.piece(self.chip_of(rel), self.core, p)
        return pltpu.make_async_remote_copy(ref, ref, self.s_link.at[SLOT[i]], self.r_link.at[i], device_id={"sp": self.to[link]})

    def came(self, i):
        link, rel, p, _, _ = COPIES[i]
        ref = self.piece(self.chip_of(_arrives_as(link, rel)), self.core, p)
        return pltpu.make_async_remote_copy(ref, ref, self.s_link.at[SLOT[i]], self.r_link.at[i], device_id={"sp": self.to[link]})

    def across(self, rel, p, core):
        i, chip = rel[0] * 8 + rel[1] * 4 + rel[2], self.chip_of(rel)
        if p is None:
            return self.block(chip, i, core)
        ref = self.piece(chip, core, p)
        return pltpu.make_async_remote_copy(ref, ref, self.s_pair.at[i], self.r_pair.at[i], device_id={"sp": self.pair})

    def block(self, chip, i, core):
        ref = self.kv.at[chip * 2 + core]
        return pltpu.make_async_remote_copy(ref, ref, self.s_pair.at[i], self.r_pair.at[i], device_id={"sp": self.pair})

    def among(self, bits):
        return (jnp.int32(bits) & self.bit) != 0

    def run(self, slot):
        for _, kind, _, i in slot:
            link, rel, p, _, _ = COPIES[i]
            if kind == 1:
                if HAD[i] is not None:
                    pl.when(self.among(SENDS[HAD[i]]))(self.link(HAD[i]).wait_send)
                pl.when(self.among(SENDS[i]))(self.link(i).start)
            else:
                here = _arrives_as(link, rel)
                pl.when(self.among(GETS[i]))(self.came(i).wait_recv)
                pl.when(self.chip_of(here) < self.chip)(self.across(here, p, self.core).start)

    def finish(self):
        for i in sorted(set(SLOT) - set(HAD.values())):
            pl.when(self.among(SENDS[i]))(self.link(i).wait_send)
        for rel in [(0, 0, 0), *RELS]:
            pl.when(self.chip_of(rel) <= self.chip)(self.across(rel, None, self.core).wait_send)


class _Softmax:
    def __init__(self, kv, q_s, top_s, mix_s, open_p, open_keep, open_s):
        self.kv, self.q_s, self.top_s, self.mix_s = kv, q_s, top_s, mix_s
        self.open_p, self.open_keep, self.open_s = open_p, open_keep, open_s

    def keys(self, chip):
        return jnp.concatenate([self.kv[2 * chip + i, 0:256, :] for i in range(2)], axis=0)

    def values(self, chip):
        v = jnp.concatenate([self.kv[2 * chip + i, 256:512, :].T for i in range(2)], axis=1)
        return jnp.concatenate([v, jnp.ones((8, 512), jnp.bfloat16)], axis=0)

    def weights(self, s, h):
        at = slice(h * OWN, (h + 1) * OWN)
        old = self.top_s[0:1, at]
        top = jnp.maximum(old, s.max(axis=0, keepdims=True))
        self.top_s[0:1, at] = top
        return jnp.exp2((s - top) * E).astype(jnp.bfloat16), jnp.exp2((old - top) * E)

    def add(self, h, v, p, keep):
        at = slice(h * OWN, (h + 1) * OWN)
        self.mix_s[:, at] = self.mix_s[:, at] * keep + _dot(v, p, 1, 0)

    def step(self, chip, before=None, visible=None):
        k, v, last = self.keys(chip), self.values(chip), HEADS - 1
        scores, done = {}, {}

        def score(h):
            s = _dot(k, self.q_s[h * OWN : (h + 1) * OWN, :], 1, 1)
            scores[h] = s if visible is None else jnp.where(visible, s, HIDDEN)

        def close(h):
            done[h] = self.weights(scores.pop(h), h)

        if before is not None:
            v_before, s_before = self.values(before), self.open_s[...]
        score(0)
        if before is not None:
            self.add(last - 1, v_before, self.open_p[...], self.open_keep[0:1, :])
            closed = self.weights(s_before, last)
        score(1)
        close(0)
        if before is not None:
            self.add(last, v_before, *closed)
        for h in range(2, HEADS):
            score(h)
            close(h - 1)
            self.add(h - 2, v, *done.pop(h - 2))
        self.open_p[...], self.open_keep[0:1, :] = done.pop(last - 1)
        self.open_s[...] = scores.pop(last)

    def finish(self, before):
        v, last = self.values(before), HEADS - 1
        self.add(last - 1, v, self.open_p[...], self.open_keep[0:1, :])
        self.add(last, v, *self.weights(self.open_s[...], last))


def _kernel(x_h, gain_h, wq_h, wk_h, wv_h, wo_h, cos_h, sin_h, base_h, seen_ref, wo_ref, x_s,
            gain_s, wq_s, wkv_s, cos_s, sin_s, base_s, a_s, q_s, kv, top_s, mix_s, open_p, open_keep, open_s, in_sem, s_link, r_link, s_pair, r_pair):
    ring = _Ring(kv, s_link, r_link, s_pair, r_pair)
    me = ring.me
    ring.greet()
    first = [(x_h.at[pl.ds(0, 128)], x_s.at[pl.ds(0, 128)]), (gain_h, gain_s), (x_h.at[pl.ds(128, 128)], x_s.at[pl.ds(128, 128)]), (cos_h, cos_s), (sin_h, sin_s), (base_h, base_s),
             (wk_h, wkv_s.at[:, pl.ds(0, HEAD)]), (wv_h, wkv_s.at[:, pl.ds(HEAD, HEAD)])]
    later = [(wq_h.at[:, pl.ds(512 * i, 512)], wq_s.at[:, pl.ds(512 * i, 512)]) for i in range(4)] + [(wo_h, wo_ref)]
    first, later = ([pltpu.make_async_copy(a, b, in_sem.at[n + i]) for i, (a, b) in enumerate(c)] for n, c in ((0, first), (8, later)))
    for c in first:
        c.start()
    for c in first[:2]:
        c.wait()
    gain = gain_s[...].astype(jnp.float32)[None]
    for at in (0, 128):
        if at:
            first[2].wait()
        wide = x_s[at : at + 128, :].astype(jnp.float32)
        scale = lax.rsqrt(jnp.mean(wide * wide, -1, keepdims=True) + 1e-6)
        a_s[at : at + 128, :] = (wide * scale * gain).astype(jnp.bfloat16)
    for c in first[3:6]:
        c.wait()
    here = base_s[me]
    cb, sb = here[:, :HALF], here[:, HALF:]
    cos = cb * cos_s[...] - sb * sin_s[...]
    sin = sb * cos_s[...] + cb * sin_s[...]
    cos_s[...] = cos
    sin_s[...] = sin
    for c in first[6:]:
        c.wait()
    for c in later[:2]:
        c.start()
    both = _dot(a_s[...], wkv_s[...], 1, 0)
    kv[me, 0:256, :] = _turn(both[:, :HEAD], cos, sin)
    kv[me, 256:512, :] = both[:, HEAD:].astype(jnp.bfloat16)

    ring.greeted()
    slots = _slots()
    for i in range(4):
        ring.run(slots[i])
        if i == 0:
            for p in range(4):
                ring.across((0, 0, 0), p, ring.core).start()
            for c in later[2:]:
                c.start()
        later[i].wait()
        for h in (2 * i, 2 * i + 1):
            q = _dot(a_s[...], wq_s[:, h * HEAD : (h + 1) * HEAD], 1, 0)
            q_s[h * OWN : (h + 1) * OWN, :] = _turn(q, cos_s[...], sin_s[...])

    ring.run(slots[4])
    top_s[...] = jnp.full(top_s.shape, NEG, jnp.float32)
    mix_s[...] = jnp.zeros(mix_s.shape, jnp.float32)
    ring.across((0, 0, 0), None, 1 - ring.core).wait_recv()
    softmax = _Softmax(kv, q_s, top_s, mix_s, open_p, open_keep, open_s)
    place = ring.core * OWN + lax.broadcasted_iota(jnp.int32, (512, OWN), 1)
    softmax.step(ring.chip, None, place >= lax.broadcasted_iota(jnp.int32, (512, OWN), 0))

    def step(n, before):
        chip = place = 0
        for i, rel in enumerate(RELS):
            chip = jnp.where(n == i, ring.chip_of(rel), chip)
            place = jnp.where(n == i, rel[0] * 8 + rel[1] * 4 + rel[2], place)
        for four in range(0, len(RELS), 4):
            @pl.when(n // 4 == four // 4)
            def _():
                for i in range(four, min(four + 4, len(RELS))):
                    if slots[5 + i]:
                        @pl.when(n == i)
                        def _():
                            ring.run(slots[5 + i])

        seen = chip < ring.chip

        @pl.when(seen)
        def _():
            ring.block(chip, place, 1 - ring.core).wait_recv()
            softmax.step(chip, before)

        return jnp.where(seen, chip, before)

    softmax.finish(lax.fori_loop(0, len(RELS), step, ring.chip))
    for h in range(HEADS):
        at = slice(h * OWN, (h + 1) * OWN)
        part = mix_s[:HEAD, at] * (1 / mix_s[HEAD : HEAD + 1, at])
        seen_ref[:, h * HEAD : (h + 1) * HEAD] = part.astype(jnp.bfloat16).T
    ring.finish()
    later[4].wait()


def _tables():
    freq = THETA ** (-np.arange(HALF) / HALF)
    place = np.arange(OWN)[:, None] * freq
    start = (np.arange(DEVICES) * OWN)[:, None] * freq
    base = np.concatenate([np.cos(start), np.sin(start)], axis=1)[:, None]
    return [jnp.asarray(t, jnp.float32) for t in (np.cos(place), np.sin(place), base)]


def _out(x_ref, seen_ref, wo_ref, y_ref, y_s, sem):
    copies = []
    for i in range(4):
        at = slice(512 * i, 512 * (i + 1))
        y = _dot(seen_ref[...], wo_ref[:, at], 1, 0)
        y_s[:, at] = (x_ref[:, at].astype(jnp.float32) + y).astype(jnp.bfloat16)
        copies.append(pltpu.make_async_copy(y_s.at[:, pl.ds(512 * i, 512)], y_ref.at[:, pl.ds(512 * i, 512)], sem.at[i]))
        copies[-1].start()
    for c in copies:
        c.wait()


def _project(x, seen, wo):
    return pl.pallas_call(
        _out,
        out_shape=jax.ShapeDtypeStruct((OWN, D), jnp.bfloat16),
        in_specs=[pl.BlockSpec(memory_space=pltpu.VMEM)] * 3,
        out_specs=pl.BlockSpec(memory_space=pl.ANY),
        scratch_shapes=[pltpu.VMEM((OWN, D), jnp.bfloat16), pltpu.SemaphoreType.DMA((4,))],
        compiler_params=pltpu.CompilerParams(vmem_limit_bytes=24 * 2**20),
        name="project",
    )(x, seen, wo)


def solution(mesh):
    def step(x, gain, wq, wk, wv, wo):
        vmem = lambda *shape: pltpu.VMEM(shape, jnp.bfloat16)
        wide = lambda *shape: pltpu.VMEM(shape, jnp.float32)
        dma = pltpu.SemaphoreType.DMA
        seen, wo, x = pl.pallas_call(
            _kernel,
            out_shape=[jax.ShapeDtypeStruct((n, D), jnp.bfloat16) for n in (OWN, D, OWN)],
            in_specs=[pl.BlockSpec(memory_space=pl.ANY)] * 9,
            out_specs=[pl.BlockSpec(memory_space=pltpu.VMEM)] * 3,
            scratch_shapes=[vmem(D), vmem(D, D), vmem(D, 2 * HEAD), wide(OWN, HALF), wide(OWN, HALF),
                            wide(DEVICES, 1, HEAD), vmem(OWN, D), vmem(COLS, HEAD), vmem(DEVICES, 2 * OWN, HEAD),
                            wide(8, COLS), wide(HEAD + 8, COLS), vmem(512, OWN), wide(8, OWN), wide(512, OWN), dma((13,)), dma((3 * RING,)), dma((len(COPIES),)), dma((16,)), dma((16,))],
            compiler_params=pltpu.CompilerParams(collective_id=0, has_side_effects=True, vmem_limit_bytes=40 * 2**20),
            cost_estimate=pl.CostEstimate(flops=2**34, bytes_accessed=2**24, transcendentals=2**24),
            name="layer",
        )(*(pltpu.with_memory_space_constraint(t, pltpu.HBM) for t in (x, gain, wq, wk, wv, wo, *_tables())))
        return _project(x, seen, wo)

    tokens, whole = P(("dp", "sp"), None), P(None, None)
    return jax.shard_map(step, mesh=mesh, in_specs=(tokens, P(None), whole, whole, whole, whole), out_specs=tokens, check_vma=False)
```
